32 devices in a mesh: blk: 8 (over z, x), field: 4 (over y, core).
Axes of the slice: x: 2, y: 2, z: 4, core: 2. Of those that a mesh axis runs over, the one named last changes fastest.
Arguments:
- vectors: float32 [512, 32768], P('blk', 'field'), may hold values from 0 to 10
- section: int32 [1], replicated, may hold values from 0 to 7
Outputs:
- metrics: float32 [512, 4, 64], P('blk', None, 'field')
The draws below stay inside these ranges and needn't reach their ends.
All inputs are finite; a program needn't handle non-finite values.
Results may differ from the reference program's by a relative error of at most 0.0003.
Values sent between devices are 32-bit elements; how exact they have to be, the bound alone decides.
A program may use at most 64 MiB of HBM per device.

```python
import math
import jax
import jax.numpy as jnp
from jax import lax

FIELDS = 32768
V_DEV = 64
STEPS = 4
VECTORS = 512
N_BLK = 8


def draw_vectors(key, part):
    folded = jax.random.fold_in(key, 17)
    key_rows, key_cols, key_cells, key_mix, key_pattern = jax.random.split(folded, 5)
    population = 8
    row_scale = jnp.exp(jax.random.uniform(key_rows, (VECTORS, 1), jnp.float32) * math.log(10.0))
    col_scale = jnp.exp(jax.random.uniform(key_cols, (1, FIELDS), jnp.float32) * math.log(10.0))
    patterns = jax.random.uniform(key_pattern, (population, FIELDS), jnp.float32)
    mixing = jax.random.uniform(key_mix, (VECTORS, population), jnp.float32) ** 4 + 0.01
    roughness = jax.random.uniform(key_cells, (VECTORS, FIELDS), jnp.float32, 0.25, 1.0)
    mixing = mixing / jnp.sum(mixing, axis=1, keepdims=True)
    blended = jnp.dot(mixing, patterns, precision=lax.Precision.HIGHEST)
    return (row_scale * col_scale * blended * roughness * 0.1).astype(jnp.float32)


def setup_inputs(seed: int = 0) -> dict:
    streams_of = jax.random.split(jax.random.key(seed), 3)
    return {
        "vectors": draw_vectors(jax.random.fold_in(streams_of[2], 71), 0),
        "section": jax.random.randint(streams_of[1], (1,), 0, N_BLK).astype(jnp.int32),
    }


def reference(vectors, section):
    sums = jnp.sum(vectors, axis=1)
    blocks = vectors.reshape(N_BLK, V_DEV, FIELDS)
    block_sums = sums.reshape(N_BLK, V_DEV)

    def one_block(index):
        own = blocks[index]
        own_sums = block_sums[index]

        def one_slot(slot):
            partner = (index + section[0] + slot) % N_BLK
            other = blocks[partner]
            other_sums = block_sums[partner]

            def one_row(row):
                return jnp.sum(jnp.minimum(row[None, :], other), axis=1)

            numer = lax.map(one_row, own)
            return 2.0 * numer / (own_sums[:, None] + other_sums[None, :])

        return lax.map(one_slot, jnp.arange(STEPS, dtype=jnp.int32))

    result = lax.map(one_block, jnp.arange(N_BLK, dtype=jnp.int32))
    return result.transpose(0, 2, 1, 3).reshape(N_BLK * V_DEV, STEPS, V_DEV)
```

```python
import functools

import jax
import jax.numpy as jnp
from jax import lax
from jax.experimental import pallas as pl
from jax.experimental.pallas import tpu as pltpu
from jax.sharding import PartitionSpec as P

STEPS = 4
LANES = 128
SUB = 8


def pair_kernel(n, groups, rows, count, sec_ref, *refs):
    pieces, before = refs[:count], refs[count:-5]
    out_ref, x_ref, turned, kept, sems = refs[-5:]
    octs = rows // SUB
    per_lane = LANES // rows
    goct = octs // groups
    numer_octs = STEPS // per_lane * goct
    sum_octs = out_ref.shape[2] - numer_octs
    chunks = x_ref.shape[2] // LANES
    lane = lax.broadcasted_iota(jnp.int32, (SUB, LANES), 1)
    offset = lax.rem(sec_ref[0], n)
    wide = min(4, octs)

    me = lax.axis_index("blk")
    copies = []
    for r, piece in enumerate(pieces):
        source = lax.rem(me + n - r, n)
        target = x_ref if count == 1 else x_ref.at[pl.ds(source * octs, octs)]
        copies.append(pltpu.make_async_copy(piece, target, sems.at[r]))
        copies[-1].start()
    for copy in copies:
        copy.wait()

    def row_total(q):
        total = x_ref[q, :, 0:LANES]
        for f in range(1, chunks):
            total += x_ref[q, :, f * LANES:(f + 1) * LANES]
        return jnp.broadcast_to(jnp.sum(total, axis=1, keepdims=True), (SUB, LANES))

    for part in range(sum_octs):
        held = jnp.zeros((SUB, LANES), jnp.float32)
        first = part * LANES
        count = min(LANES, n * octs - first)

        def add_sums(q, held):
            for u in range(8):
                held = jnp.where(lane == q * 8 + u, row_total(first + q * 8 + u), held)
            return held

        held = lax.fori_loop(0, count // 8, add_sums, held)

        def give(b, carry):
            for g in range(groups):
                out_ref[g, b, numer_octs + part] = held
            return carry

        lax.fori_loop(0, n, give, 0)

    def task(t, carry):
        slot = t // n
        b = lax.rem(t, n)
        dist = lax.rem(offset + slot, n)
        back = lax.rem(n - dist, n)
        slot2 = lax.rem(back - offset + n, n)
        k = lax.rem(b + dist, n)
        mirrored = slot2 < STEPS
        own_half = jnp.logical_or(dist == 0, b < n // 2)
        needed = jnp.logical_or(
            jnp.logical_not(mirrored),
            jnp.logical_or(slot < slot2, jnp.logical_and(slot == slot2, own_half)),
        )
        hi, lo = slot // per_lane, lax.rem(slot, per_lane)

        @pl.when(needed)
        def _():
            def finish(io):
                start = jnp.where(io >= 0, lo * rows + io * SUB, -LANES)
                for first in range(0, octs, wide):
                    for j in range(SUB):
                        mask = lane == start + j
                        for q in range(wide):
                            co = first + q
                            held = kept[j * octs + co]
                            value = jnp.broadcast_to(jnp.sum(held, axis=1, keepdims=True), (SUB, LANES))
                            pltpu.store(
                                out_ref.at[co // goct, b, hi * goct + co % goct], value, mask=mask
                            )

            def own_octet(io, carry):
                finish(io - 1)
                for first in range(0, octs, wide):
                    acc = [[None] * wide for _ in range(SUB)]
                    for f in range(chunks):
                        cols = slice(f * LANES, (f + 1) * LANES)
                        other = [x_ref[k * octs + first + q, :, cols] for q in range(wide)]
                        for j in range(SUB):
                            own = jnp.broadcast_to(x_ref[b * octs + io, j:j + 1, cols], (SUB, LANES))
                            for q in range(wide):
                                low = jnp.minimum(own, other[q])
                                acc[j][q] = low if f == 0 else acc[j][q] + low
                    for j in range(SUB):
                        for q in range(wide):
                            kept[j * octs + first + q] = acc[j][q]
                return carry

            lax.fori_loop(0, octs, own_octet, 0)
            finish(octs - 1)

            @pl.when(jnp.logical_and(mirrored, dist != 0))
            def _():
                hi2, lo2 = slot2 // per_lane, lax.rem(slot2, per_lane)
                tile = jnp.concatenate([out_ref[co // goct, b, hi * goct + co % goct] for co in range(octs)], axis=0)
                turned[...] = jnp.concatenate([tile] * per_lane, axis=0).T.reshape(turned.shape)
                mask = lane // rows == lo2
                for io in range(octs):
                    pltpu.store(
                        out_ref.at[io // goct, k, hi2 * goct + io % goct], turned[lo * octs + io], mask=mask
                    )

        return carry

    lax.fori_loop(0, STEPS * n, task, 0)
    for ref in before:
        out_ref[...] += ref[...]


def spread_kernel(n, stride, vec_ref, out_ref, held, local_sem, send_sem, recv_sem):
    me = lax.axis_index("blk")
    fields = out_ref.shape[2]
    mine = pltpu.make_async_copy(vec_ref.at[:, pl.ds(pl.multiple_of(me * stride, LANES), fields)], held, local_sem)
    mine.start()
    barrier = pltpu.get_barrier_semaphore()
    for r in range(1, n):
        pl.semaphore_signal(
            barrier, inc=1, device_id={"blk": lax.rem(me + r, n)}, device_id_type=pl.DeviceIdType.MESH
        )
    pl.semaphore_wait(barrier, n - 1)
    copies = []
    for r in sorted(range(1, n), key=lambda r: abs(2 * r - n)):
        to = lax.rem(me + r, n)
        copies.append(
            pltpu.make_async_remote_copy(
                src_ref=vec_ref.at[:, pl.ds(pl.multiple_of(to * stride, LANES), fields)],
                dst_ref=out_ref.at[me],
                send_sem=send_sem.at[r],
                recv_sem=recv_sem.at[r],
                device_id={"blk": to},
                device_id_type=pl.DeviceIdType.MESH,
            )
        )
        copies[-1].start()
    mine.wait()
    mine = pltpu.make_async_copy(held, out_ref.at[me], local_sem)
    mine.start()
    mine.wait()
    for copy in copies:
        copy.wait()


def combine_kernel(n, groups, parts_ref, out_ref, from_field, from_blk, mid, send_f, recv_f, send_b, recv_b):
    b, g = lax.axis_index("blk"), lax.axis_index("field")
    barrier = pltpu.get_barrier_semaphore()
    for r in range(1, groups):
        pl.semaphore_signal(
            barrier, inc=1, device_id={"field": lax.rem(g + r, groups)}, device_id_type=pl.DeviceIdType.MESH
        )
    for r in range(1, n):
        pl.semaphore_signal(
            barrier, inc=1, device_id={"blk": lax.rem(b + r, n)}, device_id_type=pl.DeviceIdType.MESH
        )
    pl.semaphore_wait(barrier, groups + n - 2)
    order = sorted(range(n), key=lambda r: abs(2 * r - n))
    first = {}
    for r in order:
        to = lax.rem(b + r, n)
        for h in range(1, groups):
            first[r, h] = pltpu.make_async_remote_copy(
                src_ref=parts_ref.at[lax.rem(g + h, groups), to],
                dst_ref=from_field.at[h, r],
                send_sem=send_f.at[h, r],
                recv_sem=recv_f.at[h, r],
                device_id={"field": lax.rem(g + h, groups)},
                device_id_type=pl.DeviceIdType.MESH,
            )
            first[r, h].start()
    onward = {}
    for r in order:
        to = lax.rem(b + r, n)
        total = parts_ref[g, to]
        for h in range(1, groups):
            first[r, h].wait_recv()
            total += from_field[h, r]
        mid[r] = total
        if r:
            onward[r] = pltpu.make_async_remote_copy(
                src_ref=mid.at[r],
                dst_ref=from_blk.at[r],
                send_sem=send_b.at[r],
                recv_sem=recv_b.at[r],
                device_id={"blk": to},
                device_id_type=pl.DeviceIdType.MESH,
            )
            onward[r].start()
    total = mid[0]
    for r in [r for r in order if r]:
        onward[r].wait_recv()
        total += from_blk[r]
    out_ref[...] = total
    for copy in list(first.values()) + list(onward.values()):
        copy.wait_send()


def per_device(vectors, section):
    n, groups = lax.axis_size("blk"), lax.axis_size("field")
    rows, wide = vectors.shape
    fields = wide // n
    octs = rows // SUB
    per_lane = LANES // rows
    goct = octs // groups
    numer_octs = STEPS // per_lane * goct
    sum_octs = -(-n * octs // LANES)
    octets = numer_octs + sum_octs
    early = fields

    def pairs(pieces, width, before):
        tasks = STEPS * n * rows * rows * width
        return pl.pallas_call(
            functools.partial(pair_kernel, n, groups, rows, len(pieces)),
            out_shape=jax.ShapeDtypeStruct((groups, n, octets, SUB, LANES), jnp.float32),
            in_specs=[pl.BlockSpec(memory_space=pltpu.SMEM)]
            + [pl.BlockSpec(memory_space=pl.ANY)] * len(pieces)
            + [pl.BlockSpec(memory_space=pltpu.VMEM)] * len(before),
            out_specs=pl.BlockSpec(memory_space=pltpu.VMEM),
            scratch_shapes=[
                pltpu.VMEM((n * octs, SUB, width), jnp.float32),
                pltpu.VMEM((LANES // SUB, SUB, LANES), jnp.float32),
                pltpu.VMEM((rows, SUB, LANES), jnp.float32),
                pltpu.SemaphoreType.DMA((len(pieces),)),
            ],
            cost_estimate=pl.CostEstimate(flops=2 * tasks, bytes_accessed=4 * tasks // 16, transcendentals=0),
        )(section, *pieces, *before)

    mine = pl.pallas_call(
        functools.partial(spread_kernel, n, fields),
        out_shape=jax.ShapeDtypeStruct((n, rows, early), jnp.float32),
        in_specs=[pl.BlockSpec(memory_space=pl.ANY)],
        out_specs=pl.BlockSpec(memory_space=pl.ANY),
        scratch_shapes=[
            pltpu.VMEM((rows, early), jnp.float32),
            pltpu.SemaphoreType.DMA,
            pltpu.SemaphoreType.DMA((n,)),
            pltpu.SemaphoreType.DMA((n,)),
        ],
        compiler_params=pltpu.CompilerParams(collective_id=0, has_side_effects=True),
    )(vectors)
    parts = pairs([mine.reshape(n * octs, SUB, early)], early, [])
    block = (octets, SUB, LANES)
    whole = pl.pallas_call(
        functools.partial(combine_kernel, n, groups),
        out_shape=jax.ShapeDtypeStruct(block, jnp.float32),
        in_specs=[pl.BlockSpec(memory_space=pltpu.VMEM)],
        out_specs=pl.BlockSpec(memory_space=pltpu.VMEM),
        scratch_shapes=[
            pltpu.VMEM((groups, n) + block, jnp.float32),
            pltpu.VMEM((n,) + block, jnp.float32),
            pltpu.VMEM((n,) + block, jnp.float32),
            pltpu.SemaphoreType.DMA((groups, n)),
            pltpu.SemaphoreType.DMA((groups, n)),
            pltpu.SemaphoreType.DMA((n,)),
            pltpu.SemaphoreType.DMA((n,)),
        ],
        compiler_params=pltpu.CompilerParams(collective_id=1, has_side_effects=True),
    )(parts)
    part = rows // groups
    numer = whole[:numer_octs].reshape(STEPS // per_lane, part, per_lane, rows)
    numer = numer.transpose(3, 0, 2, 1).reshape(rows, STEPS, part)
    sums = whole[numer_octs:].transpose(0, 2, 1).reshape(-1)[:n * rows].reshape(n, rows)
    b = lax.axis_index("blk")
    own = lax.dynamic_index_in_dim(sums, b, 0, keepdims=False)
    columns = lax.dynamic_slice_in_dim(sums, lax.axis_index("field") * part, part, 1)
    partner = (b + section[0] + jnp.arange(STEPS, dtype=jnp.int32)) % n
    others = columns[partner]
    return 2.0 * numer / (own[:, None, None] + others[None])


def flip(a, code, n):
    bit, total = 1, 0
    while bit < n:
        total += lax.rem(lax.rem(a // bit, 2) + lax.rem(code // bit, 2), 2) * bit
        bit *= 2
    return total


def fused_kernel(n, groups, sec_ref, vec_ref, out_ref, whole, x_ref, kept, parts, from_field, full, mid, from_blk,
                 sums_own, sums_field, sums_all, own_row, local_sem, sum_sems, spread_sems, field_sems, blk_sems):
    b, g = lax.axis_index("blk"), lax.axis_index("field")
    octs, width = x_ref.shape[1], x_ref.shape[3]
    rows = octs * SUB
    chunks = width // LANES
    wide = min(4, octs)
    lane = lax.broadcasted_iota(jnp.int32, (SUB, LANES), 1)
    sub = lax.broadcasted_iota(jnp.int32, (SUB, LANES), 0)
    low_half = lane < rows

    local = pltpu.make_async_copy(vec_ref, whole, local_sem.at[0])
    local.start()
    mine = pltpu.make_async_copy(
        vec_ref.at[:, :, pl.ds(pl.multiple_of(b * width, LANES), width)], x_ref.at[0], local_sem.at[1]
    )
    mine.start()

    blk_peer = [None] + [{"blk": flip(b, q, n)} for q in range(1, n)]
    field_peer = [None] + [{"field": lax.rem(g + h, groups)} for h in range(1, groups)]
    barrier = pltpu.get_barrier_semaphore()
    for peer in blk_peer[1:] + field_peer[1:]:
        pl.semaphore_signal(barrier, inc=1, device_id=peer, device_id_type=pl.DeviceIdType.MESH)
    pl.semaphore_wait(barrier, n + groups - 2)

    def remote(src, dst, sems, index, peer):
        return pltpu.make_async_remote_copy(
            src_ref=src, dst_ref=dst, send_sem=sems.at[(0,) + index], recv_sem=sems.at[(1,) + index],
            device_id=peer, device_id_type=pl.DeviceIdType.MESH,
        )

    spread = [None]
    for q in range(1, n):
        to = flip(b, q, n)
        spread.append(remote(
            vec_ref.at[:, :, pl.ds(pl.multiple_of(to * width, LANES), width)], x_ref.at[q], spread_sems, (q,),
            blk_peer[q],
        ))
        spread[q].start()

    local.wait()

    def row_total(o):
        total = [whole[o, :, f * LANES:(f + 1) * LANES] for f in range(4)]
        for f in range(4, whole.shape[2] // LANES):
            total[f % 4] += whole[o, :, f * LANES:(f + 1) * LANES]
        total = (total[0] + total[1]) + (total[2] + total[3])
        return jnp.broadcast_to(jnp.sum(total, axis=1, keepdims=True), (SUB, LANES))

    def add_sums(o, held):
        return jnp.where(lane == o, row_total(o), held)

    sums_own[...] = lax.fori_loop(0, octs, add_sums, jnp.zeros((SUB, LANES), jnp.float32))
    sum_f = [None]
    for h in range(1, groups):
        sum_f.append(remote(sums_own, sums_field.at[h], sum_sems, (0, h), field_peer[h]))
        sum_f[h].start()

    def finish(t, m):
        valid = m >= 0
        safe = jnp.maximum(m, 0)
        tile = t * t + safe // octs
        start = jnp.where(valid, lax.rem(safe, octs) * SUB, -4 * LANES)
        for first in range(0, octs, wide):
            for j in range(SUB):
                masks = [lane == start + j, lane == start + (j + rows)]
                for c in range(first, first + wide):
                    value = jnp.broadcast_to(jnp.sum(kept[j * octs + c], axis=1, keepdims=True), (SUB, LANES))
                    pltpu.store(parts.at[c // 2, tile], value, mask=masks[c % 2])

    def compute(t):
        def own_octet(m, carry):
            finish(t, m - 1)
            p, io = m // octs, lax.rem(m, octs)
            for first in range(0, octs, wide):
                acc = [[None] * wide for _ in range(SUB)]
                for f in range(chunks):
                    cols = slice(f * LANES, (f + 1) * LANES)
                    other = [x_ref[t, first + c, :, cols] for c in range(wide)]
                    for j in range(SUB):
                        own = jnp.broadcast_to(x_ref[p, io, j:j + 1, cols], (SUB, LANES))
                        for c in range(wide):
                            low = jnp.minimum(own, other[c])
                            acc[j][c] = low if f == 0 else acc[j][c] + low
                for j in range(SUB):
                    for c in range(wide):
                        kept[j * octs + first + c] = acc[j][c]
            return carry

        lax.fori_loop(0, (t + 1) * octs, own_octet, 0)
        finish(t, (t + 1) * octs - 1)

        def turn(p, carry):
            pieces = []
            for c in range(octs // 2):
                held = parts[c, t * t + p]
                pieces += [held, pltpu.roll(held, rows, 1)]
            tile = jnp.concatenate(pieces, axis=0)
            turned = jnp.concatenate([tile] * (LANES // rows), axis=0).T.reshape(LANES // SUB, SUB, LANES)
            for c in range(octs // 2):
                parts[c, t * t + t + 1 + p] = jnp.where(low_half, turned[2 * c], turned[2 * c + 1])
            return carry

        lax.fori_loop(0, t, turn, 0)

    gather = {}

    def reduce_field(t):
        for h in range(1, groups):
            gather[t, h].wait_recv()

        def add(i, carry):
            total = parts[g, t * t + i]
            for h in range(1, groups):
                total += from_field[h, t * t + i]
            rows_of = jnp.where(i <= t, t, i - t - 1)
            lanes_of = jnp.where(i <= t, i, t)
            full[rows_of, lanes_of] = total
            return carry

        lax.fori_loop(0, 2 * t + 1, add, 0)

    mine.wait()
    sum_b = [None]
    for t in range(n):
        if t:
            spread[t].wait_recv()
        compute(t)
        for h in range(1, groups):
            at = pl.ds(t * t, 2 * t + 1)
            gather[t, h] = remote(
                parts.at[lax.rem(g + h, groups), at], from_field.at[h, at], field_sems, (h, t), field_peer[h]
            )
            gather[t, h].start()
        if t == 0:
            total = sums_own[...]
            for h in range(1, groups):
                sum_f[h].wait_recv()
                total += sums_field[h]
            sums_all[0] = total
            for q in range(1, n):
                sum_b.append(remote(sums_all.at[0], sums_all.at[q], sum_sems, (1, q), blk_peer[q]))
                sum_b[q].start()
            held = jnp.zeros((SUB, LANES), jnp.float32)
            for o in range(octs):
                column = jnp.broadcast_to(total[:, o:o + 1], (SUB, LANES))
                pick = lax.rem(lane, rows) == o * SUB + sub
                held = jnp.where(pick, column, held)
            own_row[...] = jnp.broadcast_to(jnp.sum(held, axis=0, keepdims=True), (SUB, LANES))
        if t:
            reduce_field(t - 1)
    reduce_field(n - 1)

    offset = sec_ref[0]
    onward = {}
    for q in list(range(n - 1, 0, -1)) + [0]:
        to = flip(b, q, n)
        for s in range(STEPS):
            mid[q, s] = full[flip(b, lax.rem(to + offset + s, n), n), q]
        if q:
            onward[q] = remote(mid.at[q], from_blk.at[q], blk_sems, (q,), blk_peer[q])
            onward[q].start()

    dens = []
    for q in range(1, n):
        sum_b[q].wait_recv()
    for s in range(STEPS):
        held = sums_all[flip(b, lax.rem(b + offset + s, n), n)]
        columns = []
        for e in range(2):
            column = jnp.sum(jnp.where(lane == 2 * g + e, held, 0.0), axis=1, keepdims=True)
            columns.append(jnp.broadcast_to(column, (SUB, LANES)))
        dens.append(own_row[...] + jnp.where(low_half, columns[0], columns[1]))

    for q in range(1, n):
        onward[q].wait_recv()
    for s in range(STEPS):
        total = mid[0, s]
        for q in range(1, n):
            total += from_blk[q, s]
        value = 2.0 * total / dens[s]
        out_ref[s, 0:SUB, :] = value[:, 0:rows]
        out_ref[s, SUB:2 * SUB, :] = value[:, rows:2 * rows]
    for copy in spread[1:] + sum_f[1:] + sum_b[1:] + list(gather.values()) + list(onward.values()):
        copy.wait_send()


def fused(vectors, section):
    n, groups = lax.axis_size("blk"), lax.axis_size("field")
    rows, wide = vectors.shape
    width = wide // n
    octs = rows // SUB
    block = (SUB, LANES)
    out = pl.pallas_call(
        functools.partial(fused_kernel, n, groups),
        out_shape=jax.ShapeDtypeStruct((STEPS, rows // groups, rows), jnp.float32),
        in_specs=[pl.BlockSpec(memory_space=pltpu.SMEM), pl.BlockSpec(memory_space=pl.ANY)],
        out_specs=pl.BlockSpec(memory_space=pltpu.VMEM),
        scratch_shapes=[
            pltpu.VMEM((octs, SUB, wide), jnp.float32),
            pltpu.VMEM((n, octs, SUB, width), jnp.float32),
            pltpu.VMEM((rows,) + block, jnp.float32),
            pltpu.VMEM((groups, n * n) + block, jnp.float32),
            pltpu.VMEM((groups, n * n) + block, jnp.float32),
            pltpu.VMEM((n, n) + block, jnp.float32),
            pltpu.VMEM((n, STEPS) + block, jnp.float32),
            pltpu.VMEM((n, STEPS) + block, jnp.float32),
            pltpu.VMEM(block, jnp.float32),
            pltpu.VMEM((groups,) + block, jnp.float32),
            pltpu.VMEM((n,) + block, jnp.float32),
            pltpu.VMEM(block, jnp.float32),
            pltpu.SemaphoreType.DMA((2,)),
            pltpu.SemaphoreType.DMA((2, 2, max(n, groups))),
            pltpu.SemaphoreType.DMA((2, n)),
            pltpu.SemaphoreType.DMA((2, groups, n)),
            pltpu.SemaphoreType.DMA((2, n)),
        ],
        compiler_params=pltpu.CompilerParams(collective_id=0, has_side_effects=True),
    )(section, vectors.reshape(octs, SUB, wide))
    return out.transpose(2, 0, 1)


def any_device(vectors, section):
    n, groups = lax.axis_size("blk"), lax.axis_size("field")
    rows = vectors.shape[0]
    fits = n == 2 * STEPS and n & (n - 1) == 0 and 2 * rows == LANES and rows == 2 * SUB * groups
    return (fused if fits else per_device)(vectors, section)


def solution(mesh):
    placed = (P("blk", "field"), P())
    return jax.shard_map(
        any_device, mesh=mesh, in_specs=placed, out_specs=P("blk", None, "field"), check_vma=False
    )
```
